32 devices in a mesh: node: 16 (over z, y, x), hand: 2 (over core).
Axes of the slice: x: 2, y: 2, z: 4, core: 2. Of those that a mesh axis runs over, the one named last changes fastest.
Arguments:
- ranges: bfloat16 [512, 128, 1326], P('node', None, 'hand'), may hold values from 0.00019931793 to 0.0039978027
- strengths: int32 [512, 1326], P('node'), may hold values from 0 to 399
- live_hands: int32 [512, 1326], P('node'), may hold values 0 or 1
- pot_sizes: float32 [512, 128], P('node'), may hold values from 1 to 16
- action_counts: int32 [512], P('node'), may hold values from 1 to 8
- parents: int32 [512], P('node'), may hold values from 0 to 63
- turn_counts: int32 [16], replicated, may hold values from 1 to 4
- root_reach: float32 [16, 2, 1326], P(None, None, 'hand'), may hold values from 0.01 to 1
Outputs:
- turn_values: float32 [16, 2, 1326], P('node', None, 'hand')
- exploitability: float32 [], replicated
The draws below stay inside these ranges and needn't reach their ends.
All inputs are finite; a program needn't handle non-finite values. No bound on the sum of `live_hands` on one device may be relied on, other than what follows from the above.
Results may differ from the reference program's by a relative error of at most 0.0003.
Values may be sent and summed in bfloat16 or wider, within the bound.
A program may use at most 128 MiB of HBM per device.

```python
import math
import jax
import jax.numpy as jnp
import numpy as np
from jax import lax

H = 1326
ACT = 8
GROUPS = 8
TACT = 4
LINES = 64
NODES = 512
TURNS = 16


def with_ends(values, rng, low, high):
    longest = values.shape.index(max(values.shape))
    spots = []
    for shift in (0, 1):
        where = [jax.random.randint(jax.random.fold_in(rng, axis), (), 0, length) for axis, length in enumerate(values.shape)]
        where[longest] = (where[longest] + shift) % values.shape[longest]
        spots.append(tuple(where))
    return values.at[spots[0]].set(low).at[spots[1]].set(high)


def block_scale(rng, extent, cuts, low, top_value):
    factor_of = 1.0
    for dim, blocks in cuts:
        steps = jax.random.uniform(jax.random.fold_in(jax.random.fold_in(rng, 6), dim), (blocks,), jnp.float32, low / len(cuts), top_value / len(cuts))
        factor_of = factor_of * jnp.repeat(jnp.exp(steps), extent[dim] // blocks).reshape((-1,) + (1,) * (len(extent) - 1 - dim))
    return factor_of


def setup_inputs(seed: int = 0) -> dict:
    key_of = jax.random.split(jax.random.key(seed), 9)
    ranges = jnp.clip(jnp.exp(math.log(0.0039978027) - 2.998599 * jax.random.uniform(key_of[0], (NODES, 2 * LINES, H), jnp.float32) ** block_scale(key_of[0], (NODES, 2 * LINES, H), ((0, 16), (2, 2)), -0.2, 0.2)), 0.00019931793, 0.0039978027).astype(jnp.bfloat16)
    strengths = with_ends(jax.random.randint(key_of[1], (NODES, H), 0, 400), jax.random.fold_in(key_of[1], 1), 0, 399).astype(jnp.int32)
    live_hands = with_ends((jax.random.randint(key_of[2], (NODES, H), 0, 10) < 9).astype(jnp.int32), jax.random.fold_in(key_of[2], 1), 0, 1)
    pot_sizes = jnp.clip(jnp.exp(math.log(16.0) - 2.7725887 * jax.random.uniform(key_of[3], (NODES, 2 * LINES), jnp.float32) ** block_scale(key_of[3], (NODES, 2 * LINES), ((0, 16),), -0.2, 0.2)), 1.0, 16.0)
    action_counts = with_ends(jax.random.randint(key_of[4], (NODES,), 1, ACT + 1), jax.random.fold_in(key_of[4], 1), 1, ACT).astype(jnp.int32)
    parents = with_ends(jax.random.randint(key_of[5], (NODES,), 0, TURNS * TACT), jax.random.fold_in(key_of[5], 1), 0, (TURNS * TACT) - 1).astype(jnp.int32)
    turn_counts = with_ends(jax.random.randint(key_of[6], (TURNS,), 1, TACT + 1), jax.random.fold_in(key_of[6], 1), 1, TACT).astype(jnp.int32)
    root_reach = jnp.clip(jnp.exp(math.log(1.0) - 4.6051702 * jax.random.uniform(key_of[7], (TURNS, 2, H), jnp.float32) ** block_scale(key_of[7], (TURNS, 2, H), ((2, 2),), -0.2, 0.2)), 0.01, 1.0)
    return dict(ranges=ranges, strengths=strengths, live_hands=live_hands, pot_sizes=pot_sizes, action_counts=action_counts, parents=parents, turn_counts=turn_counts, root_reach=root_reach)


def card_pairs(wanted):
    first_list = []
    second_list = []
    for lower_card in range(52):
        for upper_card in range(lower_card + 1, 52):
            first_list.append(lower_card)
            second_list.append(upper_card)
    return (jnp.asarray(np.array(first_list[:wanted], dtype=np.int32)),
            jnp.asarray(np.array(second_list[:wanted], dtype=np.int32)))


def pair_compat(row_first, row_second, col_first, col_second):
    shared = (row_first[:, None] == col_first[None, :]) | (row_first[:, None] == col_second[None, :])
    shared = shared | (row_second[:, None] == col_first[None, :]) | (row_second[:, None] == col_second[None, :])
    return jnp.where(shared, 0.0, 1.0).astype(jnp.float32)


def reference(ranges, strengths, live_hands, pot_sizes, action_counts, parents, turn_counts, root_reach):
    first_card, second_card = card_pairs(H)
    compat = pair_compat(first_card, second_card, first_card, second_card)

    def node_best(packed):
        strength, live_row, reach_rows, pot_row, legal = packed
        live_float = live_row.astype(jnp.float32)
        signs = jnp.sign((strength[:, None] - strength[None, :]).astype(jnp.float32))
        matrix = signs * compat * live_float[:, None] * live_float[None, :]
        values = jnp.dot(reach_rows.astype(jnp.float32), matrix.T, precision=lax.Precision.HIGHEST)
        values = (values * pot_row[:, None]).reshape(2, GROUPS, ACT, H)
        usable = jnp.arange(ACT) < legal
        best = jnp.where(usable[None, None, :, None], values, -1e30).max(axis=2)
        return jnp.sum(best, axis=1)

    river_best = lax.map(node_best, (strengths, live_hands, ranges, pot_sizes, action_counts))
    sums = jax.ops.segment_sum(river_best, parents, num_segments=TURNS * TACT)
    sums = sums.reshape(TURNS, TACT, 2, H)
    usable = jnp.arange(TACT)[None, :] < turn_counts[:, None]
    turn_values = jnp.where(usable[:, :, None, None], sums, -1e30).max(axis=1)
    exploitability = jnp.sum(root_reach * turn_values)
    return turn_values, exploitability
```

```python
import functools

import jax
import jax.numpy as jnp
import numpy as np
from jax import lax
from jax.experimental import pallas as pl
from jax.experimental.pallas import tpu as pltpu
from jax.sharding import PartitionSpec as P

ACT = 8
GROUPS = 8
TACT = 4
LANE = 128
MESH = pl.DeviceIdType.MESH
GROUP = 4
MID = 200.0
LOW = -1e30


def card_rows(hands, half, padded):
    pairs = [(a, b) for a in range(52) for b in range(a + 1, 52)][:hands]
    flat = np.array(pairs, np.float32).T
    rows = np.zeros((2, 8, padded), np.float32)
    for part in range(2):
        rows[part, :2, :half] = flat[:, part * half : (part + 1) * half]
    return jnp.asarray(rows)


def kernel(
    sizes,
    ranges,
    strengths,
    live,
    pots,
    legal,
    parents,
    turn_legal,
    reach,
    cards,
    best_out,
    total_out,
    held,
    row_s,
    row_live,
    col_s,
    col_pot,
    compat,
    signs,
    lines,
    river,
    part,
    got,
    shares,
    local_sem,
    send_sem,
    recv_sem,
    out_sem,
    in_sem,
    tell_sem,
    told_sem,
):
    n_node, nodes, half, padded, turns_mine, rows_all = sizes
    f32, bf16 = jnp.float32, jnp.bfloat16
    node = lax.axis_index("node")
    hand = lax.axis_index("hand")
    me = node * 2 + hand
    n_dev = 2 * n_node
    line_cols = lines.shape[1]
    steps = nodes // GROUP

    barrier = pltpu.get_barrier_semaphore()

    def greet(offset, carry):
        other = lax.rem(me + offset, n_dev)
        pl.semaphore_signal(
            barrier,
            inc=1,
            device_id=(other // 2, lax.rem(other, 2)),
            device_id_type=MESH,
        )
        return carry

    lax.fori_loop(1, n_dev, greet, 0)

    def local_copy(step):
        span = pl.ds(step * GROUP, GROUP)
        return pltpu.make_async_copy(
            ranges.at[span], held.at[hand, span], local_sem.at[step]
        )

    def peer_copy(step):
        span = pl.ds(step * GROUP, GROUP)
        return pltpu.make_async_remote_copy(
            src_ref=ranges.at[span],
            dst_ref=held.at[hand, span],
            send_sem=send_sem.at[step],
            recv_sem=recv_sem.at[step],
            device_id=(node, 1 - hand),
            device_id_type=MESH,
        )

    for step in range(steps):
        local_copy(step).start()

    row_s[...] = jnp.zeros_like(row_s)
    strength = strengths[...].astype(f32) - MID
    alive = live[...].astype(f32)
    for side in range(2):
        cut = slice(side * half, (side + 1) * half)
        row_s[side, :nodes, :half] = strength[:, cut]
        row_s[side, nodes : nodes + 8, :] = cards[side]
        row_live[side, :, :half] = alive[:, cut]
    lines[...] = jnp.zeros_like(lines)

    pl.semaphore_wait(barrier, n_dev - 1)
    for step in range(steps):
        peer_copy(step).start()

    for side in range(2):
        for tile in range(padded // LANE):
            block = row_s[side, :, tile * LANE : (tile + 1) * LANE]
            at = side * padded + tile * LANE
            col_s[at : at + LANE, :] = block.T
    pot_block = jnp.concatenate(
        [pots[...], jnp.zeros((LANE - nodes, line_cols), f32)], axis=0
    )
    col_pot[...] = pot_block.T

    hero_first = row_s[hand, nodes : nodes + 1, :]
    hero_second = row_s[hand, nodes + 1 : nodes + 2, :]

    def compat_rows(tile, carry):
        at = pl.ds(pl.multiple_of(tile * LANE, LANE), LANE)
        first = jnp.broadcast_to(col_s[at, nodes : nodes + 1], (LANE, LANE))
        second = jnp.broadcast_to(col_s[at, nodes + 1 : nodes + 2], (LANE, LANE))
        for column in range(padded // LANE):
            cut = slice(column * LANE, (column + 1) * LANE)
            a = hero_first[:, cut]
            b = hero_second[:, cut]
            shared = (first == a) | (first == b) | (second == a) | (second == b)
            compat[at, cut] = jnp.where(shared, 0.0, 1.0).astype(bf16)
        return carry

    lax.fori_loop(0, 2 * padded // LANE, compat_rows, 0)

    def spread(row):
        tall = jnp.broadcast_to(row, (16, LANE)).astype(bf16)
        return jnp.broadcast_to(tall[None], (LANE // 16, 16, LANE)).reshape(LANE, LANE)

    action = lax.broadcasted_iota(jnp.int32, (1, ACT, padded), 1)

    def one_group(step, carry):
        local_copy(step).wait()
        peer_copy(step).wait_recv()
        for first_of in range(0, GROUP, 2):
            pair = (first_of, first_of + 1)
            for u in pair:
                n = step * GROUP + u
                for side in range(2):
                    scaled = held[side, n] * row_live[side, pl.ds(n, 1), :half].astype(bf16)
                    lines[u, :, side * padded : side * padded + half] = scaled
            hero = [row_s[hand, pl.ds(step * GROUP + u, 1), :] for u in pair]
            for tile in range(2 * padded // LANE):
                at = slice(tile * LANE, (tile + 1) * LANE)
                columns = [
                    jnp.broadcast_to(col_s[at, u : u + 1], (LANE, LANE)).astype(bf16)
                    for u in pair
                ]
                for column in range(padded // LANE):
                    cut = slice(column * LANE, (column + 1) * LANE)
                    upper = compat[at, cut]
                    lower = -upper
                    for u, hero_s, column_s in zip(pair, hero, columns):
                        gap = spread(hero_s[:, cut]) - column_s
                        signs[u, at, cut] = jnp.maximum(jnp.minimum(gap, upper), lower)
            for u in pair:
                n = step * GROUP + u
                values = jnp.dot(lines[u], signs[u], preferred_element_type=f32)
                values = values * col_pot[:, u : u + 1]
                values = values.reshape(2 * GROUPS, ACT, padded)
                values = jnp.where(action < legal[n], values, LOW)
                for shift in (4, 2, 1):
                    values = jnp.maximum(values, pltpu.roll(values, shift, 1))
                for player in range(2):
                    best = values[player * GROUPS]
                    for g in range(1, GROUPS):
                        best = best + values[player * GROUPS + g]
                    best = best[:1] * row_live[hand, pl.ds(n, 1), :]
                    river[player, pl.ds(n, 1), :] = best
        col_s[...] = pltpu.roll(col_s[...], LANE - GROUP, 1)
        col_pot[...] = pltpu.roll(col_pot[...], LANE - GROUP, 1)
        return carry

    row_live[:, :, half:] = jnp.zeros((2, nodes, padded - half), f32)
    lax.fori_loop(0, steps, one_group, 0)

    row_at = lax.broadcasted_iota(jnp.int32, (rows_all, nodes), 0)
    wanted = (row_at // (2 * TACT)) * TACT + lax.rem(row_at, TACT)
    match = parents[...] == wanted
    sums = jnp.zeros((rows_all, padded), f32)
    for player in range(2):
        mine = lax.rem(row_at // TACT, 2) == player
        chosen = jnp.where(match & mine, 1.0, 0.0).astype(bf16)
        rest = river[player]
        for _ in range(3):
            piece = rest.astype(bf16)
            sums = sums + jnp.dot(chosen, piece, preferred_element_type=f32)
            rest = rest - piece.astype(f32)
    block_rows = turns_mine * 2 * TACT
    part[...] = sums.reshape(n_node, block_rows, padded)

    def deal(offset):
        other = lax.rem(node + offset, n_node)
        return pltpu.make_async_remote_copy(
            src_ref=part.at[other],
            dst_ref=got.at[offset - 1],
            send_sem=out_sem.at[offset - 1],
            recv_sem=in_sem.at[offset - 1],
            device_id=(other, hand),
            device_id_type=MESH,
        )

    def deal_start(offset, carry):
        deal(offset).start()
        return carry

    lax.fori_loop(1, n_node, deal_start, 0)

    def add_in(offset, total):
        deal(offset).wait_recv()
        return total + got[offset - 1]

    total = lax.fori_loop(1, n_node, add_in, part[node])

    kind = lax.rem(lax.broadcasted_iota(jnp.int32, (2 * TACT, padded), 0), TACT)
    share = jnp.zeros((1, half), f32)
    for t in range(turns_mine):
        turn = node * turns_mine + t
        mine = total[t * 2 * TACT : (t + 1) * 2 * TACT]
        mine = jnp.where(kind < turn_legal[turn], mine, LOW)
        for player in range(2):
            best = jnp.max(mine[player * TACT : (player + 1) * TACT], axis=0, keepdims=True)
            best = best[:, :half]
            best_out[t, player : player + 1, :] = best
            share = share + reach[turn, player : player + 1, :] * best
    shares[me] = jnp.broadcast_to(jnp.sum(share, axis=1, keepdims=True), (8, LANE))

    def tell(offset, back):
        other = lax.rem(me + offset, n_dev)
        source = lax.rem(me + n_dev - offset, n_dev) if back else me
        return pltpu.make_async_remote_copy(
            src_ref=shares.at[me],
            dst_ref=shares.at[source],
            send_sem=tell_sem.at[offset - 1],
            recv_sem=told_sem.at[offset - 1],
            device_id=(other // 2, lax.rem(other, 2)),
            device_id_type=MESH,
        )

    def tell_start(offset, carry):
        tell(offset, False).start()
        return carry

    def tell_wait(offset, carry):
        tell(offset, True).wait_recv()
        return carry

    lax.fori_loop(1, n_dev, tell_start, 0)
    lax.fori_loop(1, n_dev, tell_wait, 0)
    whole = jnp.zeros((8, LANE), f32)
    for device in range(n_dev):
        whole = whole + shares[device]
    total_out[0, 0] = whole[0, 0]

    for step in range(steps):
        peer_copy(step).wait_send()

    def done(offset, carry):
        deal(offset).wait_send()
        return carry

    def done_tell(offset, carry):
        tell(offset, False).wait_send()
        return carry

    lax.fori_loop(1, n_node, done, 0)
    lax.fori_loop(1, n_dev, done_tell, 0)


def solution(mesh):
    n_node = mesh.shape["node"]

    def local(
        ranges, strengths, live_hands, pot_sizes, action_counts, parents, turn_counts, root_reach
    ):
        nodes, line_cols, half = ranges.shape
        hands = strengths.shape[1]
        padded = -(-half // 256) * 256
        turns_all = turn_counts.shape[0]
        turns_mine = turns_all // n_node
        rows_all = turns_all * 2 * TACT
        steps = nodes // GROUP
        f32, bf16 = jnp.float32, jnp.bfloat16
        vmem = pl.BlockSpec(memory_space=pltpu.VMEM)
        smem = pl.BlockSpec(memory_space=pltpu.SMEM)
        hbm = pl.BlockSpec(memory_space=pl.ANY)
        dma = pltpu.SemaphoreType.DMA
        best, total = pl.pallas_call(
            functools.partial(kernel, (n_node, nodes, half, padded, turns_mine, rows_all)),
            out_shape=(
                jax.ShapeDtypeStruct((turns_mine, 2, half), f32),
                jax.ShapeDtypeStruct((1, 1), f32),
            ),
            in_specs=[hbm, vmem, vmem, vmem, smem, vmem, smem, vmem, vmem],
            out_specs=(vmem, smem),
            scratch_shapes=[
                pltpu.VMEM((2, nodes, line_cols, half), bf16),
                pltpu.VMEM((2, LANE, padded), f32),
                pltpu.VMEM((2, nodes, padded), f32),
                pltpu.VMEM((2 * padded, LANE), f32),
                pltpu.VMEM((line_cols, LANE), f32),
                pltpu.VMEM((2 * padded, padded), bf16),
                pltpu.VMEM((GROUP, 2 * padded, padded), bf16),
                pltpu.VMEM((GROUP, line_cols, 2 * padded), bf16),
                pltpu.VMEM((2, nodes, padded), f32),
                pltpu.VMEM((n_node, turns_mine * 2 * TACT, padded), f32),
                pltpu.VMEM((n_node - 1, turns_mine * 2 * TACT, padded), f32),
                pltpu.VMEM((2 * n_node, 8, LANE), f32),
                dma((steps,)),
                dma((steps,)),
                dma((steps,)),
                dma((n_node - 1,)),
                dma((n_node - 1,)),
                dma((2 * n_node - 1,)),
                dma((2 * n_node - 1,)),
            ],
            compiler_params=pltpu.CompilerParams(
                collective_id=0, has_side_effects=True, vmem_limit_bytes=60 * 1024 * 1024
            ),
        )(
            ranges,
            strengths,
            live_hands,
            pot_sizes,
            action_counts,
            parents.reshape(1, nodes),
            turn_counts,
            root_reach,
            card_rows(hands, half, padded),
        )
        return best, total.reshape(())

    in_specs = (
        P("node", None, "hand"),
        P("node", None),
        P("node", None),
        P("node", None),
        P("node"),
        P("node"),
        P(),
        P(None, None, "hand"),
    )
    out_specs = (P("node", None, "hand"), P())
    return jax.shard_map(local, mesh=mesh, in_specs=in_specs, out_specs=out_specs, check_vma=False)
```
